32 devices in a mesh: gz: 8 (over z, x), gy: 4 (over y, core).
Axes of the slice: x: 2, y: 2, z: 4, core: 2. Of those that a mesh axis runs over, the one named last changes fastest.
Arguments:
- right_side: float32 [64, 32, 256], P('gz', 'gy'), may hold values from -10 to 10, as said below
Outputs:
- solution_field: float32 [64, 32, 256], P('gz', 'gy')
- residual: float32 [64, 32, 256], P('gz', 'gy')
The draws below stay inside these ranges and needn't reach their ends.
Inputs may be any that keep to these rules, and one draw needn't show every extreme that they name: `right_side`: a right-hand side.
All inputs are finite; a program needn't handle non-finite values.
Results may differ from the reference program's by a relative error of at most 0.00015.
Values sent between devices are 32-bit elements; how exact they have to be, the bound alone decides.
A program may use at most 64 MiB of HBM per device.

```python
import math
import jax
import jax.numpy as jnp

NX = 256
LEVELS = 3
NZ = 64
NY = 32


def draw_right_side(key, part):
    keys = jax.random.split(jax.random.fold_in(key, 11), 3)
    z_pos = jnp.arange(NZ, dtype=jnp.float32) / (NZ - 1)
    z_cell = jnp.arange(NZ, dtype=jnp.float32)[:, None, None]
    y_cell = jnp.arange(NY, dtype=jnp.float32)[None, :, None]
    x_cell = jnp.arange(NX, dtype=jnp.float32)[None, None, :]
    freqs = jax.random.uniform(keys[1], (4, 3), jnp.float32, 0.025, 0.1)
    phases = jax.random.uniform(keys[2], (4, 3), jnp.float32, 0.0, 2.0 * math.pi)
    smooth = jnp.zeros((NZ, NY, NX), jnp.float32)
    for term in range(4):
        smooth = smooth + 0.5 * (jnp.cos(2.0 * math.pi * freqs[term, 0] * z_cell + phases[term, 0]) * jnp.cos(2.0 * math.pi * freqs[term, 1] * y_cell + phases[term, 1]) * jnp.cos(2.0 * math.pi * freqs[term, 2] * x_cell + phases[term, 2]))
    smooth = jnp.clip(smooth, -2.0, 2.0)
    share = (0.15 + 0.85 * z_pos)[:, None, None]
    amplitude = jnp.exp(math.log(2.0) * z_pos)[:, None, None]
    noise = jnp.clip(jax.random.normal(keys[0], (NZ, NY, NX), jnp.float32), -3.5, 3.5)
    values = amplitude * (share * noise + (1.0 - share) * smooth)
    return jnp.clip(values, -10.0, 10.0).astype(jnp.float32)


def setup_inputs(seed: int = 0) -> dict:
    seeds = jax.random.split(jax.random.key(seed), 2)
    right_side = draw_right_side(jax.random.fold_in(seeds[1], 71), 0)
    return dict(right_side=right_side)


sweep_order = [((0, 0), (0, 1)), ((0, 1), (0, 1)), ((1, 0), (0, 1)), ((1, 1), (0, 1)),
               ((1, 1), (1, 0)), ((1, 0), (1, 0)), ((0, 1), (1, 0)), ((0, 0), (1, 0))]


def x_side(field):
    width = [(0, 0)] * (field.ndim - 1)
    upper = jnp.pad(field[..., 1:], width + [(0, 1)])
    lower = jnp.pad(field[..., :-1], width + [(1, 0)])
    return upper + lower


def operate(padded):
    z_cells = padded.shape[0] - 2
    y_cells = padded.shape[1] - 2
    boxed = jnp.zeros((z_cells, y_cells, padded.shape[2]), jnp.float32)
    for z_step in range(3):
        for y_step in range(3):
            boxed = boxed + padded[z_step:z_step + z_cells, y_step:y_step + y_cells, :]
    boxed = boxed + x_side(boxed)
    return 27.0 * padded[1:-1, 1:-1, :] - boxed


def group_update(padded, rhs, z_par, y_par, x_order):
    z_cells = padded.shape[0] - 2
    y_cells = padded.shape[1] - 2
    outer = None
    for z_step in (-1, 0, 1):
        for y_step in (-1, 0, 1):
            if z_step == 0 and y_step == 0:
                continue
            row = padded[1 + z_par + z_step:z_cells + z_par + z_step:2, 1 + y_par + y_step:y_cells + y_par + y_step:2, :]
            outer = row if outer is None else outer + row
    center = padded[1 + z_par:z_cells + z_par:2, 1 + y_par:y_cells + y_par:2, :]
    total = outer + x_side(outer) + rhs[z_par::2, y_par::2, :]
    parity = jnp.arange(padded.shape[2], dtype=jnp.int32) % 2
    for x_par in x_order:
        center = jnp.where(parity == x_par, (total + x_side(center)) / 26.0, center)
    return padded.at[1 + z_par:z_cells + z_par:2, 1 + y_par:y_cells + y_par:2, :].set(center)


def pad_zero(field):
    return jnp.pad(field, ((1, 1), (1, 1), (0, 0)))


def symmetric_sweeps(rhs, start):
    padded = pad_zero(start)
    for group, x_order in sweep_order:
        padded = group_update(padded, rhs, group[0], group[1], x_order)
    return padded[1:-1, 1:-1, :]


def vcycle(rhs, level):
    zeros = jnp.zeros_like(rhs)
    if level == LEVELS - 1:
        return symmetric_sweeps(rhs, zeros)
    first = symmetric_sweeps(rhs, zeros)
    defect = rhs - operate(pad_zero(first))
    coarse = vcycle(defect[::2, ::2, ::2], level + 1)
    return symmetric_sweeps(rhs, first.at[::2, ::2, ::2].add(coarse))


def reference(right_side):
    precond = vcycle(right_side, 0)
    image = operate(pad_zero(precond))
    alpha = jnp.sum(right_side * precond) / jnp.sum(precond * image)
    return alpha * precond, right_side - alpha * image
```

```python
import functools

import jax
import jax.numpy as jnp
from jax import lax
from jax.experimental import pallas as pl
from jax.experimental.pallas import tpu as pltpu
from jax.sharding import PartitionSpec as P

MESH = pl.DeviceIdType.MESH
F32 = jnp.float32

LOW0, LOW1, LOW2 = 4, 6, 2
EVENS, ODDS = 9, 8
WINDOW = EVENS + ODDS

PHASE_A = ((0, (0, 1)), (1, (0, 1)))
PHASE_B = ((0, (0, 1)), (1, (0, 1, 0)), (0, (1, 0)))
PHASE_C = ((1, (1, 0)), (0, (1, 0)))

CHUNK0 = 3
CHUNK1 = 9


def add(*terms):
    total = None
    for term in terms:
        if term is not None:
            total = term if total is None else total + term
    return total


def shift(x, axis, step):
    if x is None:
        return None
    size = x.shape[axis]
    moved = pltpu.roll(x, step % size, axis)
    index = lax.broadcasted_iota(jnp.int32, x.shape, axis)
    keep = index >= step if step > 0 else index < size + step
    return jnp.where(keep, moved, 0.0)


def pair_sum(other, parity, axis):
    return add(other, shift(other, axis, 1 if parity == 0 else -1))


def both_sides(x, axis, step):
    return add(shift(x, axis, step), shift(x, axis, -step))


def scale_rows(shape, first, count):
    row = first + 2 * lax.broadcasted_iota(jnp.int32, shape, 0)
    return jnp.where((row >= 0) & (row < count), F32(1.0 / 26.0), F32(0.0))


def box0(s):
    tall = [[add(s[yp][xp], pair_sum(s[1 - yp][xp], yp, 1)) for xp in (0, 1)] for yp in (0, 1)]
    return [[add(tall[yp][xp], pair_sum(tall[yp][1 - xp], xp, 2)) for xp in (0, 1)] for yp in (0, 1)]


def phase0(v, g, scale, steps):
    v = [list(v[0]), list(v[1])]
    for yp, order in steps:
        w = [pair_sum(v[1 - yp][xp], yp, 1) for xp in (0, 1)]
        for xp in order:
            side = pair_sum(add(w[1 - xp], v[yp][1 - xp]), xp, 2)
            v[yp][xp] = add(g[yp][xp], w[xp], side) * scale
    return v


def box1(s):
    tall = [add(s[yp], pair_sum(s[1 - yp], yp, 1)) for yp in (0, 1)]
    return [add(t, both_sides(t, 2, 1)) for t in tall]


def phase1(v, g, scale, steps):
    v = list(v)
    shape = scale.shape
    parity = lax.broadcasted_iota(jnp.int32, shape, 2) % 2
    for yp, order in steps:
        w = pair_sum(v[1 - yp], yp, 1)
        for xp in order:
            new = add(g[yp], w, both_sides(add(w, v[yp]), 2, 1)) * scale
            v[yp] = jnp.where(parity == xp, new, 0.0 if v[yp] is None else v[yp])
    return v


def box2(s):
    if s is None:
        return None
    tall = add(s, both_sides(s, 1, 1))
    return add(tall, both_sides(tall, 2, 2))


def phase2(v, g, scale, steps):
    shape = scale.shape
    y_par = lax.broadcasted_iota(jnp.int32, shape, 1) % 2
    x_par = (lax.broadcasted_iota(jnp.int32, shape, 2) // 2) % 2
    for yp, order in steps:
        w = both_sides(v, 1, 1)
        for xp in order:
            new = add(g, w, both_sides(add(w, v), 2, 2)) * scale
            v = jnp.where((y_par == yp) & (x_par == xp), new, 0.0 if v is None else v)
    return v


def chunks(low, high, size):
    for start in range(low, high, size):
        yield start, min(size, high - start)


YX = [(0, 0), (0, 1), (1, 0), (1, 1)]


def run0(v, f, z0, z_count, odd, low, high, steps, fresh):
    for at, n in chunks(low, high, CHUNK0):
        here = pl.ds(at, n)
        below, above = (pl.ds(at, n), pl.ds(at + 1, n)) if odd else (pl.ds(at - 1, n), pl.ds(at, n))
        rhs = [[f[odd][yp, xp, here] for xp in (0, 1)] for yp in (0, 1)]
        shape = rhs[0][0].shape
        scale = scale_rows(shape, z0 + 2 * at - LOW0 + odd, z_count)
        g = rhs
        if fresh > 0:
            s = [[v[1 - odd][yp, xp, below] + v[1 - odd][yp, xp, above] for xp in (0, 1)] for yp in (0, 1)]
            b = box0(s)
            g = [[rhs[yp][xp] + b[yp][xp] for xp in (0, 1)] for yp in (0, 1)]
        old = [[v[odd][yp, xp, here] if fresh > 1 else None for xp in (0, 1)] for yp in (0, 1)]
        new = phase0(old, g, scale, steps)
        for yp, xp in YX:
            v[odd][yp, xp, here] = new[yp][xp]


def run1(v, f, z0, z_count, odd, low, high, steps, fresh):
    for at, n in chunks(low, high, CHUNK1):
        here = pl.ds(at, n)
        below, above = (pl.ds(at, n), pl.ds(at + 1, n)) if odd else (pl.ds(at - 1, n), pl.ds(at, n))
        g = [f[odd, yp, here] for yp in (0, 1)]
        scale = scale_rows(g[0].shape, z0 + 2 * at - LOW1 + odd, z_count)
        if fresh > 0:
            b = box1([v[1 - odd][yp, below] + v[1 - odd][yp, above] for yp in (0, 1)])
            g = [g[yp] + b[yp] for yp in (0, 1)]
        old = [v[odd][yp, here] if fresh > 1 else None for yp in (0, 1)]
        new = phase1(old, g, scale, steps)
        for yp in (0, 1):
            v[odd][yp, here] = new[yp]


def permutation(size, inverse):
    half = size // 2
    wide = lax.broadcasted_iota(jnp.int32, (size, size), 0 if inverse else 1)
    tall = lax.broadcasted_iota(jnp.int32, (size, size), 1 if inverse else 0)
    source = jnp.where(wide < half, 2 * wide, 2 * (wide - half) + 1)
    return jnp.where(tall == source, F32(1.0), F32(0.0))


def kernel(
    gz_n, gy_n, rhs_ref, sol_ref, res_ref,
    flat, mine, got, fe, fo, ve, vo, dbuf, cmine, cgot, f1, v1e, v1o, vc, part, parts, nat,
    s1, r1, s2, r2, s3, r3,
):
    gz, gy = lax.axis_index("gz"), lax.axis_index("gy")
    zl, yl, nx = rhs_ref.shape
    y2, x2 = yl // 2, nx // 2
    yc = y2 // 2
    zc = zl // 2
    z_count = gz_n * zl
    z0 = gz * zl
    f, v = (fe, fo), (ve, vo)
    v1 = (v1e, v1o)

    def there(dz):
        return (gz + dz >= 0) & (gz + dz < gz_n)

    split = jnp.dot(
        rhs_ref[...].reshape(zl * yl, nx), permutation(nx, False),
        precision=lax.Precision.HIGHEST, preferred_element_type=F32,
    )
    for xp in (0, 1):
        flat[xp] = split[:, xp * x2 : (xp + 1) * x2]
    for z in range(zl):
        for yp, xp in YX:
            row = flat[xp, pl.ds(z * yl + yp, y2, stride=2), :]
            mine[z, (yp * 2 + xp) * y2 : (yp * 2 + xp + 1) * y2, :] = row
    got[gy, pl.ds(LOW0, zl)] = mine[...]

    @pl.when(gz == 0)
    def _():
        got[:, 0:LOW0] = jnp.zeros((gy_n, LOW0) + got.shape[2:], F32)

    @pl.when(gz == gz_n - 1)
    def _():
        got[:, LOW0 + zl :] = jnp.zeros((gy_n, WINDOW - LOW0 - zl) + got.shape[2:], F32)

    high = WINDOW - LOW0 - zl
    moves1 = {-1: (0, high, LOW0 + zl), 0: (0, zl, LOW0), 1: (zl - LOW0, LOW0, 0)}
    moves2 = {
        -2: (0, zc // 2, 7), -1: (0, zc // 2, 5), 0: (0, zc // 2, 3), 1: (0, zc // 2, 1), 2: (zc // 2 - 1, 1, 0),
    }

    def exchange(moves, source, target, ssem, rsem):
        sends, receives = [], []
        for slot, (dz, (first, n, to)) in enumerate(moves.items()):
            for dg in range(gy_n):
                if dz == 0 and dg == 0:
                    continue
                g = lax.rem(gy + dg, gy_n)
                send = pltpu.make_async_remote_copy(
                    src_ref=source.at[pl.ds(first, n)],
                    dst_ref=target.at[gy, pl.ds(to, n)],
                    send_sem=ssem.at[slot, dg],
                    recv_sem=rsem.at[slot, gy],
                    device_id=(gz + dz, g),
                    device_id_type=MESH,
                )
                receive = pltpu.make_async_remote_copy(
                    src_ref=source.at[pl.ds(first, n)],
                    dst_ref=target.at[g, pl.ds(to, n)],
                    send_sem=ssem.at[slot, dg],
                    recv_sem=rsem.at[slot, g],
                    device_id=(gz + dz, g),
                    device_id_type=MESH,
                )
                sends.append((dz, send))
                receives.append((-dz, receive))

        def each(items, act):
            for dz in sorted(moves, key=lambda d: -abs(d)):
                group = [item for at, item in items if at == dz]

                def go(group=group):
                    for item in group:
                        act(item)

                if dz == 0:
                    go()
                else:
                    pl.when(there(dz))(go)

        each(sends, lambda c: c.start())
        return lambda: (each(receives, lambda c: c.wait_recv()), each(sends, lambda c: c.wait_send()))

    exchange(moves1, mine, got, s1, r1)()

    for q in range(WINDOW):
        for k, (yp, xp) in enumerate(YX):
            for g in range(gy_n):
                f[q % 2][yp, xp, q // 2, g * y2 : (g + 1) * y2, :] = got[g, q, k * y2 : (k + 1) * y2, :]

    run0(v, f, z0, z_count, 0, 0, EVENS, PHASE_A, 0)
    run0(v, f, z0, z_count, 1, 0, ODDS, PHASE_B, 1)
    run0(v, f, z0, z_count, 0, 1, EVENS - 1, PHASE_C, 2)

    own = LOW0 // 2
    here, below, above = pl.ds(own, zc), pl.ds(own - 1, zc), pl.ds(own, zc)
    s = [[ve[yp, xp, here] + vo[yp, xp, below] + vo[yp, xp, above] for xp in (0, 1)] for yp in (0, 1)]
    tall = [s[0][xp] + pair_sum(s[1][xp], 0, 1) for xp in (0, 1)]
    dbuf[...] = fe[0, 0, here] - (27.0 * ve[0, 0, here] - (tall[0] + pair_sum(tall[1], 0, 2)))
    for z in range(zc):
        for yp in (0, 1):
            at = ((z % 2) * 2 + yp) * yc
            cmine[z // 2, at : at + yc, :] = dbuf[z, pl.ds(gy * y2 + yp, yc, stride=2), :]
    cgot[gy, pl.ds(3, zc // 2)] = cmine[...]
    for edge, low, n in ((0, 0, 3), (1, 0, 1), (gz_n - 2, 7, 2), (gz_n - 1, 5, 4)):

        @pl.when(gz == edge)
        def _(low=low, n=n):
            cgot[:, low : low + n] = jnp.zeros((gy_n, n) + cgot.shape[2:], F32)

    exchange(moves2, cmine, cgot, s2, r2)()

    for zp in (0, 1):
        for yp in (0, 1):
            at = (zp * 2 + yp) * yc
            for g in range(gy_n):
                f1[zp, yp, :, g * yc : (g + 1) * yc, :] = cgot[g, :, at : at + yc, :]

    c0, c_count = gz * zc, gz_n * zc
    run1(v1, f1, c0, c_count, 0, 0, EVENS, PHASE_A, 0)
    run1(v1, f1, c0, c_count, 1, 0, ODDS, PHASE_B, 1)
    run1(v1, f1, c0, c_count, 0, 1, EVENS - 1, PHASE_C, 2)

    f2 = []
    for i in range(1, EVENS - 1):
        s = [v1e[yp, pl.ds(i, 1)] + v1o[yp, pl.ds(i - 1, 1)] + v1o[yp, pl.ds(i, 1)] for yp in (0, 1)]
        tall = s[0] + pair_sum(s[1], 0, 1)
        f2.append(f1[0, 0, pl.ds(i, 1)] - (27.0 * v1e[0, pl.ds(i, 1)] - (tall + both_sides(tall, 2, 1))))
    q0, q_count = gz * (zc // 2), gz_n * (zc // 2)
    f2e, f2o = f2[0::2], f2[1::2]
    scale2 = [scale_rows(f2[0].shape, q0 - LOW2 + i, q_count) for i in range(7)]
    even2 = [phase2(None, f2e[k], scale2[2 * k], PHASE_A) for k in range(4)]
    odd2 = [phase2(None, f2o[k] + box2(even2[k] + even2[k + 1]), scale2[2 * k + 1], PHASE_B) for k in range(3)]
    for k in (1, 2):
        even2[k] = phase2(even2[k], f2e[k] + box2(odd2[k - 1] + odd2[k]), scale2[2 * k], PHASE_C)
    v2 = [odd2[0], even2[1], odd2[1], even2[2], odd2[2]]
    in_lane = lax.broadcasted_iota(jnp.int32, v2[0].shape, 2) % 2 == 0
    for k in range(5):
        v1e[0, pl.ds(2 + k, 1)] = v1e[0, pl.ds(2 + k, 1)] + jnp.where(in_lane, v2[k], 0.0)

    run1(v1, f1, c0, c_count, 0, 2, 7, PHASE_A, 2)
    run1(v1, f1, c0, c_count, 1, 2, 6, PHASE_B, 2)
    run1(v1, f1, c0, c_count, 0, 3, 6, PHASE_C, 2)

    half = v1e.shape[2]
    for c in range(-1, 6):
        odd = c % 2
        i = (c + LOW1 - odd) // 2
        for yp in (0, 1):
            vc[c + 1, pl.ds(yp, half, stride=2), :] = v1[odd][yp, i]
    ve[0, 0, pl.ds(1, 7)] = ve[0, 0, pl.ds(1, 7)] + vc[...]

    run0(v, f, z0, z_count, 0, 1, 8, PHASE_A, 2)
    run0(v, f, z0, z_count, 1, 1, 7, PHASE_B, 2)
    run0(v, f, z0, z_count, 0, 2, 7, PHASE_C, 2)

    numer = denom = None
    for odd in (0, 1):
        for k in range(zc):
            i = own + k
            here, below, above = pl.ds(i, 1), pl.ds(i - 1 + odd, 1), pl.ds(i + odd, 1)
            p = [[v[odd][yp, xp, here] for xp in (0, 1)] for yp in (0, 1)]
            s = [[p[yp][xp] + v[1 - odd][yp, xp, below] + v[1 - odd][yp, xp, above] for xp in (0, 1)] for yp in (0, 1)]
            b = box0(s)
            for yp, xp in YX:
                image = 27.0 * p[yp][xp] - b[yp][xp]
                numer = add(numer, f[odd][yp, xp, here] * p[yp][xp])
                denom = add(denom, p[yp][xp] * image)
                parity_at = k * 2 + odd
                nat[yp, xp, pl.ds(parity_at, 1)] = image
    rows = numer.shape[1]
    for j, total in enumerate((numer, denom)):
        acc = None
        for r in range(0, rows, 8):
            acc = add(acc, total[0, r : r + 8, :])
        part[j] = acc

    sends, receives = [], []
    for d in range(1, gz_n):
        to = lax.rem(gz + d, gz_n)
        sends.append(pltpu.make_async_remote_copy(
            src_ref=part, dst_ref=parts.at[gz], send_sem=s3.at[d], recv_sem=r3.at[gz],
            device_id=(to, gy), device_id_type=MESH,
        ))
        receives.append(pltpu.make_async_remote_copy(
            src_ref=part, dst_ref=parts.at[to], send_sem=s3.at[d], recv_sem=r3.at[to],
            device_id=(to, gy), device_id_type=MESH,
        ))
    for c in sends:
        c.start()
    parts[gz] = part[...]

    back = permutation(nx, True)
    for which, out in ((0, sol_ref), (1, res_ref)):
        for z in range(zl):
            for yp, xp in YX:
                if which == 0:
                    row = v[z % 2][yp, xp, own + z // 2, pl.ds(gy * y2, y2), :]
                else:
                    row = nat[yp, xp, z, pl.ds(gy * y2, y2), :]
                flat[xp, pl.ds(z * yl + yp, y2, stride=2), :] = row
        out[...] = jnp.dot(
            jnp.concatenate([flat[0], flat[1]], axis=1), back, precision=lax.Precision.HIGHEST, preferred_element_type=F32
        ).reshape(zl, yl, nx)

    for c in receives:
        c.wait_recv()
    for c in sends:
        c.wait_send()
    sums = parts[0]
    for d in range(1, gz_n):
        sums = sums + parts[d]
    alpha = jnp.sum(sums[0], keepdims=True) / jnp.sum(sums[1], keepdims=True)
    alpha = alpha.reshape(1, 1, 1)
    sol_ref[...] = sol_ref[...] * alpha
    res_ref[...] = rhs_ref[...] - res_ref[...] * alpha


def solution(mesh):
    gz_n, gy_n = mesh.shape["gz"], mesh.shape["gy"]

    def body(rhs):
        zl, yl, nx = rhs.shape
        y2, x2 = yl // 2, nx // 2
        y_half = gy_n * y2
        zc, yc = zl // 2, y2 // 2
        vmem = lambda *shape: pltpu.VMEM(shape, F32)
        dma = lambda *shape: pltpu.SemaphoreType.DMA(shape)
        return pl.pallas_call(
            functools.partial(kernel, gz_n, gy_n),
            out_shape=[jax.ShapeDtypeStruct(rhs.shape, F32)] * 2,
            in_specs=[pl.BlockSpec(memory_space=pltpu.VMEM)],
            out_specs=[pl.BlockSpec(memory_space=pltpu.VMEM)] * 2,
            scratch_shapes=[
                vmem(2, zl * yl, x2),
                vmem(zl, 4 * y2, x2),
                vmem(gy_n, WINDOW, 4 * y2, x2),
                vmem(2, 2, EVENS, y_half, x2),
                vmem(2, 2, ODDS, y_half, x2),
                vmem(2, 2, EVENS, y_half, x2),
                vmem(2, 2, ODDS, y_half, x2),
                vmem(zc, y_half, x2),
                vmem(zc // 2, 4 * yc, x2),
                vmem(gy_n, 9, 4 * yc, x2),
                vmem(2, 2, 9, gy_n * yc, x2),
                vmem(2, EVENS, gy_n * yc, x2),
                vmem(2, ODDS, gy_n * yc, x2),
                vmem(7, y_half, x2),
                vmem(2, 8, x2),
                vmem(gz_n, 2, 8, x2),
                vmem(2, 2, zl, y_half, x2),
                dma(3, gy_n), dma(3, gy_n), dma(5, gy_n), dma(5, gy_n), dma(gz_n), dma(gz_n),
            ],
            compiler_params=pltpu.CompilerParams(has_side_effects=True),
        )(rhs)

    return jax.shard_map(
        lambda rhs: tuple(body(rhs)),
        mesh=mesh,
        in_specs=(P("gz", "gy", None),),
        out_specs=(P("gz", "gy", None), P("gz", "gy", None)),
        check_vma=False,
    )
```

```python
import functools

import jax
import jax.numpy as jnp
from jax import lax
from jax.experimental import pallas as pl
from jax.experimental.pallas import tpu as pltpu
from jax.sharding import PartitionSpec as P

MESH = pl.DeviceIdType.MESH
F32 = jnp.float32

LOW0, LOW1, LOW2 = 4, 6, 2
EVENS, ODDS = 9, 8
WINDOW = EVENS + ODDS

PHASE_A = ((0, (0, 1)), (1, (0, 1)))
PHASE_B = ((0, (0, 1)), (1, (0, 1, 0)), (0, (1, 0)))
PHASE_C = ((1, (1, 0)), (0, (1, 0)))

CHUNK0 = 3
CHUNK1 = 9


def add(*terms):
    total = None
    for term in terms:
        if term is not None:
            total = term if total is None else total + term
    return total


def shift(x, axis, step):
    if x is None:
        return None
    size = x.shape[axis]
    moved = pltpu.roll(x, step % size, axis)
    index = lax.broadcasted_iota(jnp.int32, x.shape, axis)
    keep = index >= step if step > 0 else index < size + step
    return jnp.where(keep, moved, 0.0)


def pair_sum(other, parity, axis):
    return add(other, shift(other, axis, 1 if parity == 0 else -1))


def both_sides(x, axis, step):
    return add(shift(x, axis, step), shift(x, axis, -step))


def scale_rows(shape, first, count):
    row = first + 2 * lax.broadcasted_iota(jnp.int32, shape, 0)
    return jnp.where((row >= 0) & (row < count), F32(1.0 / 26.0), F32(0.0))


def box0(s):
    tall = [[add(s[yp][xp], pair_sum(s[1 - yp][xp], yp, 1)) for xp in (0, 1)] for yp in (0, 1)]
    return [[add(tall[yp][xp], pair_sum(tall[yp][1 - xp], xp, 2)) for xp in (0, 1)] for yp in (0, 1)]


def phase0(v, g, scale, steps):
    v = [list(v[0]), list(v[1])]
    for yp, order in steps:
        w = [pair_sum(v[1 - yp][xp], yp, 1) for xp in (0, 1)]
        for xp in order:
            side = pair_sum(add(w[1 - xp], v[yp][1 - xp]), xp, 2)
            v[yp][xp] = add(g[yp][xp], w[xp], side) * scale
    return v


def box1(s):
    tall = [add(s[yp], pair_sum(s[1 - yp], yp, 1)) for yp in (0, 1)]
    return [add(t, both_sides(t, 2, 1)) for t in tall]


def phase1(v, g, scale, steps):
    v = list(v)
    shape = scale.shape
    parity = lax.broadcasted_iota(jnp.int32, shape, 2) % 2
    for yp, order in steps:
        w = pair_sum(v[1 - yp], yp, 1)
        for xp in order:
            new = add(g[yp], w, both_sides(add(w, v[yp]), 2, 1)) * scale
            v[yp] = jnp.where(parity == xp, new, 0.0 if v[yp] is None else v[yp])
    return v


def box2(s):
    if s is None:
        return None
    tall = add(s, both_sides(s, 1, 1))
    return add(tall, both_sides(tall, 2, 2))


def phase2(v, g, scale, steps):
    shape = scale.shape
    y_par = lax.broadcasted_iota(jnp.int32, shape, 1) % 2
    x_par = (lax.broadcasted_iota(jnp.int32, shape, 2) // 2) % 2
    for yp, order in steps:
        w = both_sides(v, 1, 1)
        for xp in order:
            new = add(g, w, both_sides(add(w, v), 2, 2)) * scale
            v = jnp.where((y_par == yp) & (x_par == xp), new, 0.0 if v is None else v)
    return v


def chunks(low, high, size):
    for start in range(low, high, size):
        yield start, min(size, high - start)


YX = [(0, 0), (0, 1), (1, 0), (1, 1)]


def run0(v, f, z0, z_count, odd, low, high, steps, fresh):
    for at, n in chunks(low, high, CHUNK0):
        here = pl.ds(at, n)
        below, above = (pl.ds(at, n), pl.ds(at + 1, n)) if odd else (pl.ds(at - 1, n), pl.ds(at, n))
        rhs = [[f[odd][yp, xp, here] for xp in (0, 1)] for yp in (0, 1)]
        shape = rhs[0][0].shape
        scale = scale_rows(shape, z0 + 2 * at - LOW0 + odd, z_count)
        g = rhs
        if fresh > 0:
            s = [[v[1 - odd][yp, xp, below] + v[1 - odd][yp, xp, above] for xp in (0, 1)] for yp in (0, 1)]
            b = box0(s)
            g = [[rhs[yp][xp] + b[yp][xp] for xp in (0, 1)] for yp in (0, 1)]
        old = [[v[odd][yp, xp, here] if fresh > 1 else None for xp in (0, 1)] for yp in (0, 1)]
        new = phase0(old, g, scale, steps)
        for yp, xp in YX:
            v[odd][yp, xp, here] = new[yp][xp]


def run1(v, f, z0, z_count, odd, low, high, steps, fresh):
    for at, n in chunks(low, high, CHUNK1):
        here = pl.ds(at, n)
        below, above = (pl.ds(at, n), pl.ds(at + 1, n)) if odd else (pl.ds(at - 1, n), pl.ds(at, n))
        g = [f[odd, yp, here] for yp in (0, 1)]
        scale = scale_rows(g[0].shape, z0 + 2 * at - LOW1 + odd, z_count)
        if fresh > 0:
            b = box1([v[1 - odd][yp, below] + v[1 - odd][yp, above] for yp in (0, 1)])
            g = [g[yp] + b[yp] for yp in (0, 1)]
        old = [v[odd][yp, here] if fresh > 1 else None for yp in (0, 1)]
        new = phase1(old, g, scale, steps)
        for yp in (0, 1):
            v[odd][yp, here] = new[yp]


def permutation(size, inverse):
    half = size // 2
    wide = lax.broadcasted_iota(jnp.int32, (size, size), 0 if inverse else 1)
    tall = lax.broadcasted_iota(jnp.int32, (size, size), 1 if inverse else 0)
    source = jnp.where(wide < half, 2 * wide, 2 * (wide - half) + 1)
    return jnp.where(tall == source, F32(1.0), F32(0.0))


def kernel(
    gz_n, gy_n, rhs_ref, sol_ref, res_ref,
    flat, mine, got, fe, fo, ve, vo, dbuf, cmine, cgot, f1, v1e, v1o, vc, part, parts, nat,
    s1, r1, s2, r2, s3, r3, s4,
):
    gz, gy = lax.axis_index("gz"), lax.axis_index("gy")
    zl, yl, nx = rhs_ref.shape
    y2, x2 = yl // 2, nx // 2
    yc = y2 // 2
    zc = zl // 2
    z_count = gz_n * zl
    z0 = gz * zl
    f, v = (fe, fo), (ve, vo)
    v1 = (v1e, v1o)

    def there(dz):
        return (gz + dz >= 0) & (gz + dz < gz_n)

    barrier = pltpu.get_barrier_semaphore()
    count = jnp.int32(0)
    for dz in range(1 - gz_n, gz_n):
        for dg in range(gy_n if abs(dz) <= 2 else 1):
            if dz == 0 and dg == 0:
                continue

            @pl.when(there(dz))
            def _(dz=dz, dg=dg):
                pl.semaphore_signal(
                    barrier, inc=1, device_id=(gz + dz, lax.rem(gy + dg, gy_n)), device_id_type=MESH
                )

            count = count + there(dz).astype(jnp.int32)

    split = jnp.dot(
        rhs_ref[...].reshape(zl * yl, nx), permutation(nx, False),
        precision=lax.Precision.HIGHEST, preferred_element_type=F32,
    )
    for xp in (0, 1):
        flat[xp] = split[:, xp * x2 : (xp + 1) * x2]
    for z in range(zl):
        for yp, xp in YX:
            row = flat[xp, pl.ds(z * yl + yp, y2, stride=2), :]
            mine[z, (yp * 2 + xp) * y2 : (yp * 2 + xp + 1) * y2, :] = row
    got[gy, pl.ds(LOW0, zl)] = mine[...]

    @pl.when(gz == 0)
    def _():
        got[:, 0:LOW0] = jnp.zeros((gy_n, LOW0) + got.shape[2:], F32)

    @pl.when(gz == gz_n - 1)
    def _():
        got[:, LOW0 + zl :] = jnp.zeros((gy_n, WINDOW - LOW0 - zl) + got.shape[2:], F32)

    high = WINDOW - LOW0 - zl
    moves1 = {-1: (0, high, LOW0 + zl), 0: (0, zl, LOW0), 1: (zl - LOW0, LOW0, 0)}
    moves2 = {
        -2: (0, zc // 2, 7), -1: (0, zc // 2, 5), 0: (0, zc // 2, 3), 1: (0, zc // 2, 1), 2: (zc // 2 - 1, 1, 0),
    }

    order1 = [
        (slot, dz, h) for h in range(gy_n // 2) for slot, dz in ((2, 0), (0, 1), (1, -1)) if dz != 0 or h != 0
    ]

    def gather():
        sibling = gy + 1 - 2 * lax.rem(gy, 2)

        def blocks(act):
            for slot, dz in enumerate((1, -1, 0)):
                for h in range(gy_n // 2):
                    if dz == 0 and h == 0:
                        continue
                    act(slot, dz, h)

        def when_there(dz, go):
            if dz == 0:
                go()
            else:
                pl.when(there(dz))(go)

        def direct(slot, dz, h, owner):
            first, n, to = moves1[dz]
            g = lax.rem(gy + 2 * h, gy_n)
            return pltpu.make_async_remote_copy(
                src_ref=mine.at[pl.ds(first, n)],
                dst_ref=got.at[g if owner else gy, pl.ds(to, n)],
                send_sem=s1.at[slot, h],
                recv_sem=r1.at[slot, g if owner else gy],
                device_id=(gz - dz if owner else gz + dz, g),
                device_id_type=MESH,
            )

        def relay(slot, dz, h, owner):
            _, n, to = moves1[dz]
            g = lax.rem((sibling if owner else gy) + 2 * h, gy_n)
            place = got.at[g, pl.ds(to, n)]
            return pltpu.make_async_remote_copy(
                src_ref=mine if dz == 0 and h == 0 else place,
                dst_ref=place,
                send_sem=s4.at[slot, h],
                recv_sem=r1.at[slot, g],
                device_id=(gz, sibling),
                device_id_type=MESH,
            )

        blocks(lambda slot, dz, h: when_there(dz, lambda: direct(slot, dz, h, False).start()))
        relay(2, 0, 0, False).start()

        def forward(slot, dz, h):
            def go():
                direct(slot, dz, h, True).wait_recv()
                relay(slot, dz, h, False).start()

            when_there(-dz, go)

        for slot, dz, h in order1:
            forward(slot, dz, h)
        relay(2, 0, 0, True).wait_recv()
        for slot, dz, h in order1:
            when_there(-dz, lambda: relay(slot, dz, h, True).wait_recv())
        relay(2, 0, 0, False).wait_send()
        for slot, dz, h in order1:
            when_there(-dz, lambda: relay(slot, dz, h, False).wait_send())
        blocks(lambda slot, dz, h: when_there(dz, lambda: direct(slot, dz, h, False).wait_send()))

    def exchange(moves, source, target, ssem, rsem):
        sends, receives = [], []
        for slot, (dz, (first, n, to)) in enumerate(moves.items()):
            for dg in range(gy_n):
                if dz == 0 and dg == 0:
                    continue
                g = lax.rem(gy + dg, gy_n)
                send = pltpu.make_async_remote_copy(
                    src_ref=source.at[pl.ds(first, n)],
                    dst_ref=target.at[gy, pl.ds(to, n)],
                    send_sem=ssem.at[slot, dg],
                    recv_sem=rsem.at[slot, gy],
                    device_id=(gz + dz, g),
                    device_id_type=MESH,
                )
                receive = pltpu.make_async_remote_copy(
                    src_ref=source.at[pl.ds(first, n)],
                    dst_ref=target.at[g, pl.ds(to, n)],
                    send_sem=ssem.at[slot, dg],
                    recv_sem=rsem.at[slot, g],
                    device_id=(gz + dz, g),
                    device_id_type=MESH,
                )
                sends.append((dz, send))
                receives.append((-dz, receive))

        def each(items, act):
            for dz in sorted(moves, key=lambda d: -abs(d)):
                group = [item for at, item in items if at == dz]

                def go(group=group):
                    for item in group:
                        act(item)

                if dz == 0:
                    go()
                else:
                    pl.when(there(dz))(go)

        each(sends, lambda c: c.start())
        return lambda: (each(receives, lambda c: c.wait_recv()), each(sends, lambda c: c.wait_send()))

    pl.semaphore_wait(barrier, count)
    gather()

    for q in range(WINDOW):
        for k, (yp, xp) in enumerate(YX):
            for g in range(gy_n):
                f[q % 2][yp, xp, q // 2, g * y2 : (g + 1) * y2, :] = got[g, q, k * y2 : (k + 1) * y2, :]

    run0(v, f, z0, z_count, 0, 0, EVENS, PHASE_A, 0)
    run0(v, f, z0, z_count, 1, 0, ODDS, PHASE_B, 1)
    run0(v, f, z0, z_count, 0, 1, EVENS - 1, PHASE_C, 2)

    own = LOW0 // 2
    here, below, above = pl.ds(own, zc), pl.ds(own - 1, zc), pl.ds(own, zc)
    s = [[ve[yp, xp, here] + vo[yp, xp, below] + vo[yp, xp, above] for xp in (0, 1)] for yp in (0, 1)]
    tall = [s[0][xp] + pair_sum(s[1][xp], 0, 1) for xp in (0, 1)]
    dbuf[...] = fe[0, 0, here] - (27.0 * ve[0, 0, here] - (tall[0] + pair_sum(tall[1], 0, 2)))
    for z in range(zc):
        for yp in (0, 1):
            at = ((z % 2) * 2 + yp) * yc
            cmine[z // 2, at : at + yc, :] = dbuf[z, pl.ds(gy * y2 + yp, yc, stride=2), :]
    cgot[gy, pl.ds(3, zc // 2)] = cmine[...]
    for edge, low, n in ((0, 0, 3), (1, 0, 1), (gz_n - 2, 7, 2), (gz_n - 1, 5, 4)):

        @pl.when(gz == edge)
        def _(low=low, n=n):
            cgot[:, low : low + n] = jnp.zeros((gy_n, n) + cgot.shape[2:], F32)

    exchange(moves2, cmine, cgot, s2, r2)()

    for zp in (0, 1):
        for yp in (0, 1):
            at = (zp * 2 + yp) * yc
            for g in range(gy_n):
                f1[zp, yp, :, g * yc : (g + 1) * yc, :] = cgot[g, :, at : at + yc, :]

    c0, c_count = gz * zc, gz_n * zc
    run1(v1, f1, c0, c_count, 0, 0, EVENS, PHASE_A, 0)
    run1(v1, f1, c0, c_count, 1, 0, ODDS, PHASE_B, 1)
    run1(v1, f1, c0, c_count, 0, 1, EVENS - 1, PHASE_C, 2)

    f2 = []
    for i in range(1, EVENS - 1):
        s = [v1e[yp, pl.ds(i, 1)] + v1o[yp, pl.ds(i - 1, 1)] + v1o[yp, pl.ds(i, 1)] for yp in (0, 1)]
        tall = s[0] + pair_sum(s[1], 0, 1)
        f2.append(f1[0, 0, pl.ds(i, 1)] - (27.0 * v1e[0, pl.ds(i, 1)] - (tall + both_sides(tall, 2, 1))))
    q0, q_count = gz * (zc // 2), gz_n * (zc // 2)
    f2e, f2o = f2[0::2], f2[1::2]
    scale2 = [scale_rows(f2[0].shape, q0 - LOW2 + i, q_count) for i in range(7)]
    even2 = [phase2(None, f2e[k], scale2[2 * k], PHASE_A) for k in range(4)]
    odd2 = [phase2(None, f2o[k] + box2(even2[k] + even2[k + 1]), scale2[2 * k + 1], PHASE_B) for k in range(3)]
    for k in (1, 2):
        even2[k] = phase2(even2[k], f2e[k] + box2(odd2[k - 1] + odd2[k]), scale2[2 * k], PHASE_C)
    v2 = [odd2[0], even2[1], odd2[1], even2[2], odd2[2]]
    in_lane = lax.broadcasted_iota(jnp.int32, v2[0].shape, 2) % 2 == 0
    for k in range(5):
        v1e[0, pl.ds(2 + k, 1)] = v1e[0, pl.ds(2 + k, 1)] + jnp.where(in_lane, v2[k], 0.0)

    run1(v1, f1, c0, c_count, 0, 2, 7, PHASE_A, 2)
    run1(v1, f1, c0, c_count, 1, 2, 6, PHASE_B, 2)
    run1(v1, f1, c0, c_count, 0, 3, 6, PHASE_C, 2)

    half = v1e.shape[2]
    for c in range(-1, 6):
        odd = c % 2
        i = (c + LOW1 - odd) // 2
        for yp in (0, 1):
            vc[c + 1, pl.ds(yp, half, stride=2), :] = v1[odd][yp, i]
    ve[0, 0, pl.ds(1, 7)] = ve[0, 0, pl.ds(1, 7)] + vc[...]

    run0(v, f, z0, z_count, 0, 1, 8, PHASE_A, 2)
    run0(v, f, z0, z_count, 1, 1, 7, PHASE_B, 2)
    run0(v, f, z0, z_count, 0, 2, 7, PHASE_C, 2)

    numer = denom = None
    for odd in (0, 1):
        for k in range(zc):
            i = own + k
            here, below, above = pl.ds(i, 1), pl.ds(i - 1 + odd, 1), pl.ds(i + odd, 1)
            p = [[v[odd][yp, xp, here] for xp in (0, 1)] for yp in (0, 1)]
            s = [[p[yp][xp] + v[1 - odd][yp, xp, below] + v[1 - odd][yp, xp, above] for xp in (0, 1)] for yp in (0, 1)]
            b = box0(s)
            for yp, xp in YX:
                image = 27.0 * p[yp][xp] - b[yp][xp]
                numer = add(numer, f[odd][yp, xp, here] * p[yp][xp])
                denom = add(denom, p[yp][xp] * image)
                parity_at = k * 2 + odd
                nat[yp, xp, pl.ds(parity_at, 1)] = image
    rows = numer.shape[1]
    for j, total in enumerate((numer, denom)):
        acc = None
        for r in range(0, rows, 8):
            acc = add(acc, total[0, r : r + 8, :])
        part[pl.ds(j, 1), :] = jnp.sum(acc, axis=0, keepdims=True)

    sends, receives = [], []
    for d in range(1, gz_n):
        to = lax.rem(gz + d, gz_n)
        sends.append(pltpu.make_async_remote_copy(
            src_ref=part, dst_ref=parts.at[gz], send_sem=s3.at[d], recv_sem=r3.at[gz],
            device_id=(to, gy), device_id_type=MESH,
        ))
        receives.append(pltpu.make_async_remote_copy(
            src_ref=part, dst_ref=parts.at[to], send_sem=s3.at[d], recv_sem=r3.at[to],
            device_id=(to, gy), device_id_type=MESH,
        ))
    for c in sends:
        c.start()
    parts[gz] = part[...]

    back = permutation(nx, True)
    for which, out in ((0, sol_ref), (1, res_ref)):
        for z in range(zl):
            for yp, xp in YX:
                if which == 0:
                    row = v[z % 2][yp, xp, own + z // 2, pl.ds(gy * y2, y2), :]
                else:
                    row = nat[yp, xp, z, pl.ds(gy * y2, y2), :]
                flat[xp, pl.ds(z * yl + yp, y2, stride=2), :] = row
        out[...] = jnp.dot(
            jnp.concatenate([flat[0], flat[1]], axis=1), back, precision=lax.Precision.HIGHEST, preferred_element_type=F32
        ).reshape(zl, yl, nx)

    for c in receives:
        c.wait_recv()
    for c in sends:
        c.wait_send()
    sums = parts[0]
    for d in range(1, gz_n):
        sums = sums + parts[d]
    alpha = jnp.sum(sums[0:1], axis=1, keepdims=True) / jnp.sum(sums[1:2], axis=1, keepdims=True)
    alpha = alpha.reshape(1, 1, 1)
    sol_ref[...] = sol_ref[...] * alpha
    res_ref[...] = rhs_ref[...] - res_ref[...] * alpha


def solution(mesh):
    gz_n, gy_n = mesh.shape["gz"], mesh.shape["gy"]

    def body(rhs):
        zl, yl, nx = rhs.shape
        y2, x2 = yl // 2, nx // 2
        y_half = gy_n * y2
        zc, yc = zl // 2, y2 // 2
        vmem = lambda *shape: pltpu.VMEM(shape, F32)
        dma = lambda *shape: pltpu.SemaphoreType.DMA(shape)
        return pl.pallas_call(
            functools.partial(kernel, gz_n, gy_n),
            out_shape=[jax.ShapeDtypeStruct(rhs.shape, F32)] * 2,
            in_specs=[pl.BlockSpec(memory_space=pltpu.VMEM)],
            out_specs=[pl.BlockSpec(memory_space=pltpu.VMEM)] * 2,
            scratch_shapes=[
                vmem(2, zl * yl, x2),
                vmem(zl, 4 * y2, x2),
                vmem(gy_n, WINDOW, 4 * y2, x2),
                vmem(2, 2, EVENS, y_half, x2),
                vmem(2, 2, ODDS, y_half, x2),
                vmem(2, 2, EVENS, y_half, x2),
                vmem(2, 2, ODDS, y_half, x2),
                vmem(zc, y_half, x2),
                vmem(zc // 2, 4 * yc, x2),
                vmem(gy_n, 9, 4 * yc, x2),
                vmem(2, 2, 9, gy_n * yc, x2),
                vmem(2, EVENS, gy_n * yc, x2),
                vmem(2, ODDS, gy_n * yc, x2),
                vmem(7, y_half, x2),
                vmem(2, x2),
                vmem(gz_n, 2, x2),
                vmem(2, 2, zl, y_half, x2),
                dma(3, gy_n), dma(3, gy_n), dma(5, gy_n), dma(5, gy_n), dma(gz_n), dma(gz_n), dma(3, gy_n),
            ],
            compiler_params=pltpu.CompilerParams(has_side_effects=True, collective_id=0),
        )(rhs)

    return jax.shard_map(
        lambda rhs: tuple(body(rhs)),
        mesh=mesh,
        in_specs=(P("gz", "gy", None),),
        out_specs=(P("gz", "gy", None), P("gz", "gy", None)),
        check_vma=False,
    )
```

```python
import functools

import jax
import jax.numpy as jnp
from jax import lax
from jax.experimental import pallas as pl
from jax.experimental.pallas import tpu as pltpu
from jax.sharding import PartitionSpec as P

MESH = pl.DeviceIdType.MESH
F32 = jnp.float32

LOW0, LOW1, LOW2 = 4, 6, 2
EVENS, ODDS = 9, 8
WINDOW = EVENS + ODDS

PHASE_A = ((0, (0, 1)), (1, (0, 1)))
PHASE_B = ((0, (0, 1)), (1, (0, 1, 0)), (0, (1, 0)))
PHASE_C = ((1, (1, 0)), (0, (1, 0)))

CHUNK0 = 3
CHUNK1 = 9


def add(*terms):
    total = None
    for term in terms:
        if term is not None:
            total = term if total is None else total + term
    return total


def shift(x, axis, step):
    if x is None:
        return None
    size = x.shape[axis]
    moved = pltpu.roll(x, step % size, axis)
    index = lax.broadcasted_iota(jnp.int32, x.shape, axis)
    keep = index >= step if step > 0 else index < size + step
    return jnp.where(keep, moved, 0.0)


def pair_sum(other, parity, axis):
    return add(other, shift(other, axis, 1 if parity == 0 else -1))


def both_sides(x, axis, step):
    return add(shift(x, axis, step), shift(x, axis, -step))


def scale_rows(shape, first, count):
    row = first + 2 * lax.broadcasted_iota(jnp.int32, shape, 0)
    return jnp.where((row >= 0) & (row < count), F32(1.0 / 26.0), F32(0.0))


def box0(s):
    tall = [[add(s[yp][xp], pair_sum(s[1 - yp][xp], yp, 1)) for xp in (0, 1)] for yp in (0, 1)]
    return [[add(tall[yp][xp], pair_sum(tall[yp][1 - xp], xp, 2)) for xp in (0, 1)] for yp in (0, 1)]


def phase0(v, g, scale, steps):
    v = [list(v[0]), list(v[1])]
    for yp, order in steps:
        w = [pair_sum(v[1 - yp][xp], yp, 1) for xp in (0, 1)]
        for xp in order:
            side = pair_sum(add(w[1 - xp], v[yp][1 - xp]), xp, 2)
            v[yp][xp] = add(g[yp][xp], w[xp], side) * scale
    return v


def box1(s):
    tall = [add(s[yp], pair_sum(s[1 - yp], yp, 1)) for yp in (0, 1)]
    return [add(t, both_sides(t, 2, 1)) for t in tall]


def phase1(v, g, scale, steps):
    v = list(v)
    shape = scale.shape
    parity = lax.broadcasted_iota(jnp.int32, shape, 2) % 2
    for yp, order in steps:
        w = pair_sum(v[1 - yp], yp, 1)
        for xp in order:
            new = add(g[yp], w, both_sides(add(w, v[yp]), 2, 1)) * scale
            v[yp] = jnp.where(parity == xp, new, 0.0 if v[yp] is None else v[yp])
    return v


def box2(s):
    if s is None:
        return None
    tall = add(s, both_sides(s, 1, 1))
    return add(tall, both_sides(tall, 2, 2))


def phase2(v, g, scale, steps):
    shape = scale.shape
    y_par = lax.broadcasted_iota(jnp.int32, shape, 1) % 2
    x_par = (lax.broadcasted_iota(jnp.int32, shape, 2) // 2) % 2
    for yp, order in steps:
        w = both_sides(v, 1, 1)
        for xp in order:
            new = add(g, w, both_sides(add(w, v), 2, 2)) * scale
            v = jnp.where((y_par == yp) & (x_par == xp), new, 0.0 if v is None else v)
    return v


def chunks(low, high, size):
    for start in range(low, high, size):
        yield start, min(size, high - start)


YX = [(0, 0), (0, 1), (1, 0), (1, 1)]


def run0(v, f, z0, z_count, odd, low, high, steps, fresh):
    for at, n in chunks(low, high, CHUNK0):
        here = pl.ds(at, n)
        below, above = (pl.ds(at, n), pl.ds(at + 1, n)) if odd else (pl.ds(at - 1, n), pl.ds(at, n))
        rhs = [[f[odd][yp, xp, here] for xp in (0, 1)] for yp in (0, 1)]
        shape = rhs[0][0].shape
        scale = scale_rows(shape, z0 + 2 * at - LOW0 + odd, z_count)
        g = rhs
        if fresh > 0:
            s = [[v[1 - odd][yp, xp, below] + v[1 - odd][yp, xp, above] for xp in (0, 1)] for yp in (0, 1)]
            b = box0(s)
            g = [[rhs[yp][xp] + b[yp][xp] for xp in (0, 1)] for yp in (0, 1)]
        old = [[v[odd][yp, xp, here] if fresh > 1 else None for xp in (0, 1)] for yp in (0, 1)]
        new = phase0(old, g, scale, steps)
        for yp, xp in YX:
            v[odd][yp, xp, here] = new[yp][xp]


def run1(v, f, z0, z_count, odd, low, high, steps, fresh):
    for at, n in chunks(low, high, CHUNK1):
        here = pl.ds(at, n)
        below, above = (pl.ds(at, n), pl.ds(at + 1, n)) if odd else (pl.ds(at - 1, n), pl.ds(at, n))
        g = [f[odd, yp, here] for yp in (0, 1)]
        scale = scale_rows(g[0].shape, z0 + 2 * at - LOW1 + odd, z_count)
        if fresh > 0:
            b = box1([v[1 - odd][yp, below] + v[1 - odd][yp, above] for yp in (0, 1)])
            g = [g[yp] + b[yp] for yp in (0, 1)]
        old = [v[odd][yp, here] if fresh > 1 else None for yp in (0, 1)]
        new = phase1(old, g, scale, steps)
        for yp in (0, 1):
            v[odd][yp, here] = new[yp]


def permutation(size, inverse):
    half = size // 2
    wide = lax.broadcasted_iota(jnp.int32, (size, size), 0 if inverse else 1)
    tall = lax.broadcasted_iota(jnp.int32, (size, size), 1 if inverse else 0)
    source = jnp.where(wide < half, 2 * wide, 2 * (wide - half) + 1)
    return jnp.where(tall == source, F32(1.0), F32(0.0))


def kernel(
    gz_n, gy_n, rhs_hbm, sol_ref, res_ref,
    flat, mine, got, fe, fo, ve, vo, dbuf, cmine, cgot, f1, v1e, v1o, vc, part, parts, nat,
    s1, r1, s2, r2, s3, r3, s4, rhs_ref, s5,
):
    gz, gy = lax.axis_index("gz"), lax.axis_index("gy")
    zl, yl, nx = rhs_ref.shape
    fetch = pltpu.make_async_copy(rhs_hbm, rhs_ref, s5)
    fetch.start()
    y2, x2 = yl // 2, nx // 2
    yc = y2 // 2
    zc = zl // 2
    z_count = gz_n * zl
    z0 = gz * zl
    f, v = (fe, fo), (ve, vo)
    v1 = (v1e, v1o)

    def there(dz):
        return (gz + dz >= 0) & (gz + dz < gz_n)

    barrier = pltpu.get_barrier_semaphore()
    count = jnp.int32(0)
    for dz in range(1 - gz_n, gz_n):
        for dg in range(gy_n if abs(dz) <= 2 else 1):
            if dz == 0 and dg == 0:
                continue

            @pl.when(there(dz))
            def _(dz=dz, dg=dg):
                pl.semaphore_signal(
                    barrier, inc=1, device_id=(gz + dz, lax.rem(gy + dg, gy_n)), device_id_type=MESH
                )

            count = count + there(dz).astype(jnp.int32)

    fetch.wait()
    split = jnp.dot(
        rhs_ref[...].reshape(zl * yl, nx), permutation(nx, False),
        precision=lax.Precision.HIGHEST, preferred_element_type=F32,
    )
    for xp in (0, 1):
        flat[xp] = split[:, xp * x2 : (xp + 1) * x2]
    for z in range(zl):
        for yp, xp in YX:
            row = flat[xp, pl.ds(z * yl + yp, y2, stride=2), :]
            mine[z, (yp * 2 + xp) * y2 : (yp * 2 + xp + 1) * y2, :] = row
    got[gy, pl.ds(LOW0, zl)] = mine[...]

    @pl.when(gz == 0)
    def _():
        got[:, 0:LOW0] = jnp.zeros((gy_n, LOW0) + got.shape[2:], F32)

    @pl.when(gz == gz_n - 1)
    def _():
        got[:, LOW0 + zl :] = jnp.zeros((gy_n, WINDOW - LOW0 - zl) + got.shape[2:], F32)

    high = WINDOW - LOW0 - zl
    moves1 = {-1: (0, high, LOW0 + zl), 0: (0, zl, LOW0), 1: (zl - LOW0, LOW0, 0)}
    moves2 = {
        -2: (0, zc // 2, 7), -1: (0, zc // 2, 5), 0: (0, zc // 2, 3), 1: (0, zc // 2, 1), 2: (zc // 2 - 1, 1, 0),
    }

    order1 = [
        (slot, dz, h) for h in range(gy_n // 2) for slot, dz in ((2, 0), (0, 1), (1, -1)) if dz != 0 or h != 0
    ]

    def gather():
        sibling = gy + 1 - 2 * lax.rem(gy, 2)

        def blocks(act):
            for slot, dz in enumerate((1, -1, 0)):
                for h in range(gy_n // 2):
                    if dz == 0 and h == 0:
                        continue
                    act(slot, dz, h)

        def when_there(dz, go):
            if dz == 0:
                go()
            else:
                pl.when(there(dz))(go)

        def direct(slot, dz, h, owner):
            first, n, to = moves1[dz]
            g = lax.rem(gy + 2 * h, gy_n)
            return pltpu.make_async_remote_copy(
                src_ref=mine.at[pl.ds(first, n)],
                dst_ref=got.at[g if owner else gy, pl.ds(to, n)],
                send_sem=s1.at[slot, h],
                recv_sem=r1.at[slot, g if owner else gy],
                device_id=(gz - dz if owner else gz + dz, g),
                device_id_type=MESH,
            )

        def relay(slot, dz, h, owner):
            _, n, to = moves1[dz]
            g = lax.rem((sibling if owner else gy) + 2 * h, gy_n)
            place = got.at[g, pl.ds(to, n)]
            return pltpu.make_async_remote_copy(
                src_ref=mine if dz == 0 and h == 0 else place,
                dst_ref=place,
                send_sem=s4.at[slot, h],
                recv_sem=r1.at[slot, g],
                device_id=(gz, sibling),
                device_id_type=MESH,
            )

        blocks(lambda slot, dz, h: when_there(dz, lambda: direct(slot, dz, h, False).start()))
        relay(2, 0, 0, False).start()

        def forward(slot, dz, h):
            def go():
                direct(slot, dz, h, True).wait_recv()
                relay(slot, dz, h, False).start()

            when_there(-dz, go)

        for slot, dz, h in order1:
            forward(slot, dz, h)
        relay(2, 0, 0, True).wait_recv()
        for slot, dz, h in order1:
            when_there(-dz, lambda: relay(slot, dz, h, True).wait_recv())
        relay(2, 0, 0, False).wait_send()
        for slot, dz, h in order1:
            when_there(-dz, lambda: relay(slot, dz, h, False).wait_send())
        blocks(lambda slot, dz, h: when_there(dz, lambda: direct(slot, dz, h, False).wait_send()))

    def exchange(moves, source, target, ssem, rsem):
        sends, receives = [], []
        for slot, (dz, (first, n, to)) in enumerate(moves.items()):
            for dg in range(gy_n):
                if dz == 0 and dg == 0:
                    continue
                g = lax.rem(gy + dg, gy_n)
                send = pltpu.make_async_remote_copy(
                    src_ref=source.at[pl.ds(first, n)],
                    dst_ref=target.at[gy, pl.ds(to, n)],
                    send_sem=ssem.at[slot, dg],
                    recv_sem=rsem.at[slot, gy],
                    device_id=(gz + dz, g),
                    device_id_type=MESH,
                )
                receive = pltpu.make_async_remote_copy(
                    src_ref=source.at[pl.ds(first, n)],
                    dst_ref=target.at[g, pl.ds(to, n)],
                    send_sem=ssem.at[slot, dg],
                    recv_sem=rsem.at[slot, g],
                    device_id=(gz + dz, g),
                    device_id_type=MESH,
                )
                sends.append((dz, send))
                receives.append((-dz, receive))

        def each(items, act):
            for dz in sorted(moves, key=lambda d: -abs(d)):
                group = [item for at, item in items if at == dz]

                def go(group=group):
                    for item in group:
                        act(item)

                if dz == 0:
                    go()
                else:
                    pl.when(there(dz))(go)

        each(sends, lambda c: c.start())
        return lambda: (each(receives, lambda c: c.wait_recv()), each(sends, lambda c: c.wait_send()))

    pl.semaphore_wait(barrier, count)
    gather()

    for q in range(WINDOW):
        for k, (yp, xp) in enumerate(YX):
            for g in range(gy_n):
                f[q % 2][yp, xp, q // 2, g * y2 : (g + 1) * y2, :] = got[g, q, k * y2 : (k + 1) * y2, :]

    run0(v, f, z0, z_count, 0, 0, EVENS, PHASE_A, 0)
    run0(v, f, z0, z_count, 1, 0, ODDS, PHASE_B, 1)
    run0(v, f, z0, z_count, 0, 1, EVENS - 1, PHASE_C, 2)

    own = LOW0 // 2
    here, below, above = pl.ds(own, zc), pl.ds(own - 1, zc), pl.ds(own, zc)
    s = [[ve[yp, xp, here] + vo[yp, xp, below] + vo[yp, xp, above] for xp in (0, 1)] for yp in (0, 1)]
    tall = [s[0][xp] + pair_sum(s[1][xp], 0, 1) for xp in (0, 1)]
    dbuf[...] = fe[0, 0, here] - (27.0 * ve[0, 0, here] - (tall[0] + pair_sum(tall[1], 0, 2)))
    for z in range(zc):
        for yp in (0, 1):
            at = ((z % 2) * 2 + yp) * yc
            cmine[z // 2, at : at + yc, :] = dbuf[z, pl.ds(gy * y2 + yp, yc, stride=2), :]
    cgot[gy, pl.ds(3, zc // 2)] = cmine[...]
    for edge, low, n in ((0, 0, 3), (1, 0, 1), (gz_n - 2, 7, 2), (gz_n - 1, 5, 4)):

        @pl.when(gz == edge)
        def _(low=low, n=n):
            cgot[:, low : low + n] = jnp.zeros((gy_n, n) + cgot.shape[2:], F32)

    exchange(moves2, cmine, cgot, s2, r2)()

    for zp in (0, 1):
        for yp in (0, 1):
            at = (zp * 2 + yp) * yc
            for g in range(gy_n):
                f1[zp, yp, :, g * yc : (g + 1) * yc, :] = cgot[g, :, at : at + yc, :]

    c0, c_count = gz * zc, gz_n * zc
    run1(v1, f1, c0, c_count, 0, 0, EVENS, PHASE_A, 0)
    run1(v1, f1, c0, c_count, 1, 0, ODDS, PHASE_B, 1)
    run1(v1, f1, c0, c_count, 0, 1, EVENS - 1, PHASE_C, 2)

    f2 = []
    for i in range(1, EVENS - 1):
        s = [v1e[yp, pl.ds(i, 1)] + v1o[yp, pl.ds(i - 1, 1)] + v1o[yp, pl.ds(i, 1)] for yp in (0, 1)]
        tall = s[0] + pair_sum(s[1], 0, 1)
        f2.append(f1[0, 0, pl.ds(i, 1)] - (27.0 * v1e[0, pl.ds(i, 1)] - (tall + both_sides(tall, 2, 1))))
    q0, q_count = gz * (zc // 2), gz_n * (zc // 2)
    f2e, f2o = f2[0::2], f2[1::2]
    scale2 = [scale_rows(f2[0].shape, q0 - LOW2 + i, q_count) for i in range(7)]
    even2 = [phase2(None, f2e[k], scale2[2 * k], PHASE_A) for k in range(4)]
    odd2 = [phase2(None, f2o[k] + box2(even2[k] + even2[k + 1]), scale2[2 * k + 1], PHASE_B) for k in range(3)]
    for k in (1, 2):
        even2[k] = phase2(even2[k], f2e[k] + box2(odd2[k - 1] + odd2[k]), scale2[2 * k], PHASE_C)
    v2 = [odd2[0], even2[1], odd2[1], even2[2], odd2[2]]
    in_lane = lax.broadcasted_iota(jnp.int32, v2[0].shape, 2) % 2 == 0
    for k in range(5):
        v1e[0, pl.ds(2 + k, 1)] = v1e[0, pl.ds(2 + k, 1)] + jnp.where(in_lane, v2[k], 0.0)

    run1(v1, f1, c0, c_count, 0, 2, 7, PHASE_A, 2)
    run1(v1, f1, c0, c_count, 1, 2, 6, PHASE_B, 2)
    run1(v1, f1, c0, c_count, 0, 3, 6, PHASE_C, 2)

    half = v1e.shape[2]
    for c in range(-1, 6):
        odd = c % 2
        i = (c + LOW1 - odd) // 2
        for yp in (0, 1):
            vc[c + 1, pl.ds(yp, half, stride=2), :] = v1[odd][yp, i]
    ve[0, 0, pl.ds(1, 7)] = ve[0, 0, pl.ds(1, 7)] + vc[...]

    run0(v, f, z0, z_count, 0, 1, 8, PHASE_A, 2)
    run0(v, f, z0, z_count, 1, 1, 7, PHASE_B, 2)
    run0(v, f, z0, z_count, 0, 2, 7, PHASE_C, 2)

    numer = denom = None
    for odd in (0, 1):
        for k in range(zc):
            i = own + k
            here, below, above = pl.ds(i, 1), pl.ds(i - 1 + odd, 1), pl.ds(i + odd, 1)
            p = [[v[odd][yp, xp, here] for xp in (0, 1)] for yp in (0, 1)]
            s = [[p[yp][xp] + v[1 - odd][yp, xp, below] + v[1 - odd][yp, xp, above] for xp in (0, 1)] for yp in (0, 1)]
            b = box0(s)
            for yp, xp in YX:
                image = 27.0 * p[yp][xp] - b[yp][xp]
                numer = add(numer, f[odd][yp, xp, here] * p[yp][xp])
                denom = add(denom, p[yp][xp] * image)
                parity_at = k * 2 + odd
                nat[yp, xp, pl.ds(parity_at, 1)] = image
    rows = numer.shape[1]
    for j, total in enumerate((numer, denom)):
        acc = None
        for r in range(0, rows, 8):
            acc = add(acc, total[0, r : r + 8, :])
        part[pl.ds(j, 1), :] = jnp.sum(acc, axis=0, keepdims=True)

    sends, receives = [], []
    for d in range(1, gz_n):
        to = lax.rem(gz + d, gz_n)
        sends.append(pltpu.make_async_remote_copy(
            src_ref=part, dst_ref=parts.at[gz], send_sem=s3.at[d], recv_sem=r3.at[gz],
            device_id=(to, gy), device_id_type=MESH,
        ))
        receives.append(pltpu.make_async_remote_copy(
            src_ref=part, dst_ref=parts.at[to], send_sem=s3.at[d], recv_sem=r3.at[to],
            device_id=(to, gy), device_id_type=MESH,
        ))
    for c in sends:
        c.start()
    parts[gz] = part[...]

    back = permutation(nx, True)
    for which, out in ((0, sol_ref), (1, res_ref)):
        for z in range(zl):
            for yp, xp in YX:
                if which == 0:
                    row = v[z % 2][yp, xp, own + z // 2, pl.ds(gy * y2, y2), :]
                else:
                    row = nat[yp, xp, z, pl.ds(gy * y2, y2), :]
                flat[xp, pl.ds(z * yl + yp, y2, stride=2), :] = row
        out[...] = jnp.dot(
            jnp.concatenate([flat[0], flat[1]], axis=1), back, precision=lax.Precision.HIGHEST, preferred_element_type=F32
        ).reshape(zl, yl, nx)

    for c in receives:
        c.wait_recv()
    for c in sends:
        c.wait_send()
    sums = parts[0]
    for d in range(1, gz_n):
        sums = sums + parts[d]
    alpha = jnp.sum(sums[0:1], axis=1, keepdims=True) / jnp.sum(sums[1:2], axis=1, keepdims=True)
    alpha = alpha.reshape(1, 1, 1)
    sol_ref[...] = sol_ref[...] * alpha
    res_ref[...] = rhs_ref[...] - res_ref[...] * alpha


def solution(mesh):
    gz_n, gy_n = mesh.shape["gz"], mesh.shape["gy"]

    def body(rhs):
        zl, yl, nx = rhs.shape
        y2, x2 = yl // 2, nx // 2
        y_half = gy_n * y2
        zc, yc = zl // 2, y2 // 2
        vmem = lambda *shape: pltpu.VMEM(shape, F32)
        dma = lambda *shape: pltpu.SemaphoreType.DMA(shape)
        return pl.pallas_call(
            functools.partial(kernel, gz_n, gy_n),
            out_shape=[jax.ShapeDtypeStruct(rhs.shape, F32)] * 2,
            in_specs=[pl.BlockSpec(memory_space=pl.ANY)],
            out_specs=[pl.BlockSpec(memory_space=pltpu.VMEM)] * 2,
            scratch_shapes=[
                vmem(2, zl * yl, x2),
                vmem(zl, 4 * y2, x2),
                vmem(gy_n, WINDOW, 4 * y2, x2),
                vmem(2, 2, EVENS, y_half, x2),
                vmem(2, 2, ODDS, y_half, x2),
                vmem(2, 2, EVENS, y_half, x2),
                vmem(2, 2, ODDS, y_half, x2),
                vmem(zc, y_half, x2),
                vmem(zc // 2, 4 * yc, x2),
                vmem(gy_n, 9, 4 * yc, x2),
                vmem(2, 2, 9, gy_n * yc, x2),
                vmem(2, EVENS, gy_n * yc, x2),
                vmem(2, ODDS, gy_n * yc, x2),
                vmem(7, y_half, x2),
                vmem(2, x2),
                vmem(gz_n, 2, x2),
                vmem(2, 2, zl, y_half, x2),
                dma(3, gy_n), dma(3, gy_n), dma(5, gy_n), dma(5, gy_n), dma(gz_n), dma(gz_n), dma(3, gy_n),
                vmem(zl, yl, nx), pltpu.SemaphoreType.DMA,
            ],
            compiler_params=pltpu.CompilerParams(has_side_effects=True, collective_id=0),
        )(rhs)

    return jax.shard_map(
        lambda rhs: tuple(body(rhs)),
        mesh=mesh,
        in_specs=(P("gz", "gy", None),),
        out_specs=(P("gz", "gy", None), P("gz", "gy", None)),
        check_vma=False,
    )
```
